32 devices in a mesh: terms: 2 (over x), rows: 4 (over y, core), cols: 4 (over z).
Axes of the slice: x: 2, y: 2, z: 4, core: 2. Of those that a mesh axis runs over, the one named last changes fastest.
Arguments:
- wavefunction: bfloat16 [2, 1024, 1024], P(None, 'rows', 'cols'), may hold values from -6 to 6
- energy: float32 [2], replicated, may hold values from 1 to 4
- block_rows: int32 [2], replicated, may hold values from 512 to 1024
- block_cols: int32 [2], replicated, may hold values from 512 to 1024
- left_ops: bfloat16 [8, 1024, 1024], P('terms', 'rows'), may hold values from -0.1875 to 0.1875
- right_ops: bfloat16 [8, 1024, 1024], P('terms', 'cols'), may hold values from -0.1875 to 0.1875
- source: int32 [8], P('terms'), may hold values from 0 to 1
- target: int32 [8], P('terms'), may hold values from 0 to 1
Outputs:
- sigma: bfloat16 [2, 1024, 1024], P(None, 'rows', 'cols')
- residual: bfloat16 [2, 1024, 1024], P(None, 'rows', 'cols')
The draws below stay inside these ranges and needn't reach their ends.
Inputs may be any that keep to these rules, and one draw needn't show every extreme that they name: source[t] is the sector whose block term t reads. target[t] is the sector to which term t adds. `block_rows`: entries of a sector block beyond its live left or right states are ignored.
All inputs are finite; a program needn't handle non-finite values.
Results may differ from the reference program's by a relative error of at most 0.0044.
The reference program's roundings to bfloat16 on the way count: a program that leaves them out, or rounds other values in their place, can miss the bound.
Values may be sent and summed in bfloat16 or wider, within the bound.
No kernel may reach another device: no remote copies, remote signals or barrier semaphores. Data moves between devices by JAX's collectives and lax.ppermute only.
A program may use at most 64 MiB of HBM per device.

```python
import math
import jax
import jax.numpy as jnp
import numpy as np
from jax import lax

BLK = 1024
NSEC = 2
TERMS = 8


def plant(array, own_key, smallest, top_value):
    shape = array.shape
    index_at = [jax.random.randint(jax.random.fold_in(own_key, axis), (), 0, shape[axis]) for axis in range(len(shape))]
    array = array.at[tuple(index_at)].set(smallest)
    longest = shape.index(max(shape))
    index_at[longest] = (index_at[longest] + 1) % shape[longest]
    return array.at[tuple(index_at)].set(top_value)


def block_scale(key, dims, pieces, least, largest):
    factor_of, own = 1.0, jax.random.fold_in(key, 6)
    for axis_at, parts in pieces:
        steps = jnp.exp(jax.random.uniform(jax.random.fold_in(own, axis_at), (parts,), jnp.float32, least / len(pieces), largest / len(pieces)))
        factor_of = factor_of * jnp.repeat(steps, dims[axis_at] // parts).reshape([-1 if axis == axis_at else 1 for axis in range(len(dims))])
    return factor_of


def cumulative_ranks(count, slope):
    weights = [(1 << 20) // math.isqrt(standing ** slope) + 1 for standing in range(1, count + 1)]
    scale = 1 + sum(weights) // (1 << 30)
    return np.cumsum(np.array([max(1, weight // scale) for weight in weights]))


def skewed_ids(rng, dims, amount, slope):
    listing = cumulative_ranks(amount, slope)
    ticket = jax.random.randint(jax.random.fold_in(rng, 1), dims, 0, int(listing[amount - 1]))
    rank = jnp.searchsorted(jnp.asarray(listing, jnp.int32), ticket, side="right")
    return jax.random.permutation(jax.random.fold_in(rng, 2), amount)[rank].astype(jnp.int32)


def bell_draw(stream_key, extent, scale, bound, cuts=(), kind=jnp.bfloat16):
    array = jax.random.normal(stream_key, extent, jnp.float32) * scale
    if len(cuts) > 0:
        array = block_scale(stream_key, extent, cuts, -0.22, 0.18) * array
    return jnp.clip(array, min=-bound, max=bound).astype(kind)


def setup_inputs(seed: int = 0) -> dict:
    seeds = jax.random.split(jax.random.key(seed), 9)
    return {
        "wavefunction": bell_draw(seeds[0], (NSEC, BLK, BLK), 1.0, 6.0, ((1, 4), (2, 4))),
        "energy": jnp.clip(jnp.exp(jax.random.uniform(seeds[1], (NSEC,), jnp.float32, math.log(1.0), math.log(4.0))), 1.0, 4.0),
        "block_rows": jax.random.randint(seeds[2], (NSEC,), BLK // 2, BLK + 1).astype(jnp.int32),
        "block_cols": jax.random.randint(seeds[3], (NSEC,), BLK // 2, BLK + 1).astype(jnp.int32),
        "left_ops": bell_draw(seeds[4], (TERMS, BLK, BLK), BLK ** -0.5, 0.1875, ((0, 2), (1, 4))),
        "right_ops": bell_draw(seeds[5], (TERMS, BLK, BLK), BLK ** -0.5, 0.1875, ((0, 2), (1, 4))),
        "source": plant(jax.random.randint(seeds[6], (TERMS,), 0, NSEC), jax.random.fold_in(seeds[6], 1), 0, NSEC - 1).astype(jnp.int32),
        "target": plant(skewed_ids(seeds[7], (TERMS,), NSEC, 2), jax.random.fold_in(seeds[7], 3), 0, NSEC - 1).astype(jnp.int32),
    }


def reference(wavefunction, energy, block_rows, block_cols, left_ops, right_ops, source, target):
    positions = jnp.arange(BLK, dtype=jnp.int32)
    inside = (positions[None, :, None] < block_rows[:, None, None]) & (positions[None, None, :] < block_cols[:, None, None])
    live_psi = jnp.where(inside, wavefunction, jnp.zeros_like(wavefunction))
    sector_ids = jnp.arange(NSEC, dtype=jnp.int32)

    def add_term(running, scanned):
        left_op, right_op, src_sector, dst_sector = scanned
        src_block = lax.dynamic_index_in_dim(live_psi, src_sector, 0, keepdims=False)
        products = jnp.dot(left_op, src_block, preferred_element_type=jnp.float32).astype(jnp.bfloat16)
        addition = lax.dot_general(products, right_op, (((1,), (1,)), ((), ())), preferred_element_type=jnp.float32)
        hit = (sector_ids == dst_sector)[:, None, None]
        return running + jnp.where(hit, addition[None], jnp.zeros_like(addition[None])), None

    start_sum = jnp.zeros((NSEC, BLK, BLK), jnp.float32)
    summed, unused = lax.scan(add_term, start_sum, (left_ops, right_ops, source, target))
    live_f = live_psi.astype(jnp.float32)
    full_sigma = jnp.where(inside, summed + energy[:, None, None] * live_f, jnp.zeros_like(summed))
    numerator = jnp.sum(live_f * full_sigma)
    denominator = jnp.sum(live_f * live_f)
    rayleigh = numerator / (denominator + 1e-6)
    residual = full_sigma - rayleigh * live_f
    return full_sigma.astype(jnp.bfloat16), residual.astype(jnp.bfloat16)
```

```python
import functools

import jax
import jax.numpy as jnp
from jax import lax
from jax.experimental import pallas as pl
from jax.experimental.pallas import tpu as pltpu
from jax.sharding import PartitionSpec as P

EPSILON = 1e-06
F32 = jnp.float32
BF16 = jnp.bfloat16
VMEM = pl.BlockSpec(memory_space=pltpu.VMEM)
SMEM = pl.BlockSpec(memory_space=pltpu.SMEM)


def swap(value, axis, size, bit):
    return lax.ppermute(value, axis, [(i, i ^ bit) for i in range(size)])


def shift(value, axis, size, step):
    return lax.ppermute(value, axis, [(i, (i + step) % size) for i in range(size)])


def masked(block, rows_left, cols_left):
    rows, cols = block.shape
    inside = (lax.broadcasted_iota(jnp.int32, (rows, cols), 0) < rows_left) & (
        lax.broadcasted_iota(jnp.int32, (rows, cols), 1) < cols_left
    )
    return jnp.where(inside, block.astype(F32), 0.0)


def right_kernel(cols_n, source, block_rows, block_cols, own, *refs):
    steps = cols_n - 1
    near, far = refs[:steps], refs[steps : 2 * steps]
    right, out, panel = refs[2 * steps :]
    sectors, rows, cols = own.shape
    row0 = lax.axis_index("rows") * rows
    me = lax.axis_index("cols")
    mine = lax.rem(lax.axis_index("terms"), 2)
    for s in range(sectors):
        panel[s, :, pl.ds(pl.multiple_of(me * cols, cols), cols)] = masked(
            own[s], block_rows[s] - row0, block_cols[s] - me * cols
        ).astype(BF16)
    for k in range(1, cols_n):
        at = lax.rem(me - k + cols_n, cols_n)
        for ref, s in ((near[k - 1], mine), (far[k - 1], 1 - mine)):
            panel[s, :, pl.ds(pl.multiple_of(at * cols, cols), cols)] = masked(
                ref[...], block_rows[s] - row0, block_cols[s] - at * cols
            ).astype(BF16)
    for t in range(right.shape[0]):
        out[t] = lax.dot_general(
            panel[source[t]], right[t], (((1,), (1,)), ((), ())), preferred_element_type=F32
        ).astype(BF16)


def left_kernel(rows_n, target, block_rows, block_cols, energy, own, left, *refs):
    parts = refs[:rows_n]
    out, sums, acc = refs[rows_n:]
    sectors, rows, cols = own.shape
    me = lax.axis_index("rows")
    row0 = me * rows
    col0 = lax.axis_index("cols") * cols
    acc[...] = jnp.zeros_like(acc)
    for t in range(left.shape[0]):
        total = None
        for j in range(rows_n):
            at = pl.multiple_of((me ^ j) * rows, rows)
            part = jnp.dot(left[t, :, pl.ds(at, rows)], parts[j][t], preferred_element_type=F32)
            total = part if total is None else total + part
        acc[target[t]] += total
    upper = jnp.zeros((8, 128), F32)
    steady = jnp.zeros((8, 128), F32)
    lower = jnp.zeros((8, 128), F32)
    fold = lambda v: v.reshape(rows // 8, 8, cols // 128, 128).sum((0, 2))
    for s in range(sectors):
        share = acc[s].astype(BF16)
        out[s] = share
        live = masked(own[s], block_rows[s] - row0, block_cols[s] - col0)
        upper = upper + fold(live * share.astype(F32))
        square = fold(live * live)
        steady = steady + energy[s] * square
        lower = lower + square
    sums[0] = upper
    sums[1] = steady
    sums[2] = lower


def last_kernel(block_rows, block_cols, energy, own, here, there, sums, sigma, residual):
    sectors, rows, cols = own.shape
    row0 = lax.axis_index("rows") * rows
    col0 = lax.axis_index("cols") * cols
    rayleigh = (jnp.sum(sums[0]) + jnp.sum(sums[1])) / (jnp.sum(sums[2]) + EPSILON)
    for s in range(sectors):
        live = masked(own[s], block_rows[s] - row0, block_cols[s] - col0)
        full = masked(
            here[s].astype(F32) + there[s].astype(F32), block_rows[s] - row0, block_cols[s] - col0
        ) + energy[s] * live
        sigma[s] = full.astype(BF16)
        residual[s] = (full - rayleigh * live).astype(BF16)


def sum_rows_cols(value, rows_n, cols_n):
    for axis, size in (("rows", rows_n), ("cols", cols_n)):
        bit = 1
        while bit < size:
            value = value + swap(value, axis, size, bit)
            bit *= 2
    return value


def per_device(
    terms_n, rows_n, cols_n, wavefunction, energy, block_rows, block_cols, left, right, source, target
):
    sectors, rows, cols = wavefunction.shape
    terms = left.shape[0]
    mine = lax.rem(lax.axis_index("terms"), 2)
    half = lax.dynamic_index_in_dim(wavefunction, mine, 0, keepdims=False)
    near = [shift(half, "cols", cols_n, k) for k in range(1, cols_n)]
    far = [swap(block, "terms", terms_n, 1) for block in near]
    right_part = pl.pallas_call(
        functools.partial(right_kernel, cols_n),
        out_shape=jax.ShapeDtypeStruct((terms, rows, cols), BF16),
        in_specs=[SMEM] * 3 + [VMEM] * (2 * cols_n),
        out_specs=VMEM,
        scratch_shapes=[pltpu.VMEM((sectors, rows, cols * cols_n), BF16)],
    )(source, block_rows, block_cols, wavefunction, *near, *far, right)
    parts = {0: right_part}
    bit = rows_n // 2
    while bit:
        parts.update({j ^ bit: swap(v, "rows", rows_n, bit) for j, v in list(parts.items())})
        bit //= 2
    share, sums = pl.pallas_call(
        functools.partial(left_kernel, rows_n),
        out_shape=(
            jax.ShapeDtypeStruct((sectors, rows, cols), BF16),
            jax.ShapeDtypeStruct((3, 8, 128), F32),
        ),
        in_specs=[SMEM] * 4 + [VMEM] * (2 + rows_n),
        out_specs=(VMEM, VMEM),
        scratch_shapes=[pltpu.VMEM((sectors, rows, cols), F32)],
    )(target, block_rows, block_cols, energy, wavefunction, left, *[parts[j] for j in range(rows_n)])
    if terms_n == 2:
        others = swap(share, "terms", terms_n, 1)
        sums = sums.at[0].add(swap(sums[0], "terms", terms_n, 1))
    else:
        total = lax.psum(share.astype(F32), "terms")
        others = total - share.astype(F32)
        sums = sums.at[0].set(lax.psum(sums[0], "terms"))
    sums = sum_rows_cols(sums, rows_n, cols_n)
    return pl.pallas_call(
        last_kernel,
        out_shape=(jax.ShapeDtypeStruct((sectors, rows, cols), BF16),) * 2,
        in_specs=[SMEM] * 3 + [VMEM] * 4,
        out_specs=(VMEM, VMEM),
    )(block_rows, block_cols, energy, wavefunction, share, others, sums)


def solution(mesh):
    sizes = tuple(mesh.shape[a] for a in ("terms", "rows", "cols"))
    in_specs = (
        P(None, "rows", "cols"),
        P(),
        P(),
        P(),
        P("terms", "rows", None),
        P("terms", "cols", None),
        P("terms"),
        P("terms"),
    )
    out_specs = (P(None, "rows", "cols"), P(None, "rows", "cols"))
    return jax.shard_map(
        functools.partial(per_device, *sizes),
        mesh=mesh,
        in_specs=in_specs,
        out_specs=out_specs,
        check_vma=False,
    )
```
